128 devices in a mesh: wall: 64 (over z, y, x), stream: 2 (over core).
Axes of the slice: x: 4, y: 4, z: 4, core: 2. Of those that a mesh axis runs over, the one named last changes fastest.
Arguments:
- fields: float32 [5, 2, 12288, 2048], P(None, None, 'wall', 'stream'), may hold values from -5 to 5
- wall_velocity: float32 [2, 12288, 2048], P(None, 'wall', 'stream'), may hold values from -6 to 6
- diffusion: float32 [5], replicated, may hold values from 0.5 to 16
Outputs:
- tendency: float32 [5, 2, 12288, 2048], P(None, None, 'wall', 'stream')
- advanced: float32 [5, 2, 12288, 2048], P(None, None, 'wall', 'stream')
The draws below stay inside these ranges and needn't reach their ends.
All inputs are finite; a program needn't handle non-finite values.
Results may differ from the reference program's by a relative error of at most 0.000094.
Values sent between devices are 32-bit elements; how exact they have to be, the bound alone decides.
No kernel may reach another device: no remote copies, remote signals or barrier semaphores. Data moves between devices by JAX's collectives and lax.ppermute only.
A program may use at most 128 MiB of HBM per device.

```python
import math
import jax
import jax.numpy as jnp
from jax import lax

FIELDS = 5
Z = 2
NX = 2048
NY = 12288


def draw_fields(key, part):
    first_key = jax.random.fold_in(jax.random.fold_in(key, 11), 0)
    return jnp.clip(jax.random.normal(first_key, (FIELDS, Z, NY, NX), jnp.float32), -5.0, 5.0)


def level_of(rng, dims, cuts, low, high):
    factor_of, own = 1.0, jax.random.fold_in(rng, 6)
    for axis_at, blocks in cuts:
        steps = jnp.exp(jax.random.uniform(jax.random.fold_in(own, axis_at), (blocks,), jnp.float32, low / len(cuts), high / len(cuts)))
        factor_of = factor_of * jnp.repeat(steps, dims[axis_at] // blocks).reshape([-1 if axis == axis_at else 1 for axis in range(len(dims))])
    return factor_of


def noise(rng, extent, spread, most, shards=(), kind=jnp.bfloat16):
    gain = level_of(rng, extent, shards, -0.22, 0.18) if shards else 1.0
    array = jax.random.normal(rng, extent, jnp.float32) * spread * gain
    return jnp.minimum(jnp.maximum(array, -most), most).astype(kind)


def setup_inputs(seed: int = 0) -> dict:
    key_of = jax.random.split(jax.random.key(seed), 4)
    return {
        "fields": draw_fields(jax.random.fold_in(key_of[3], 71), 0),
        "wall_velocity": noise(key_of[1], (Z, NY, NX), 1.0, 6.0, ((1, 64), (2, 2)), jnp.float32),
        "diffusion": jnp.clip(jnp.exp(jax.random.uniform(key_of[2], (FIELDS,), jnp.float32, math.log(0.5), math.log(16.0))), 0.5, 16.0),
    }


compact_alpha = 1.0 / 3.0
compact_near = 14.0 / 9.0
compact_far = 1.0 / 9.0
time_step = 0.25

def banded_solve(band, centre, source):
    planes, height, width = source.shape
    ones = jnp.ones((height,), dtype=source.dtype)
    lower = (band * ones).at[0].set(0.0)
    upper = (band * ones).at[height - 1].set(0.0)
    middle = centre * ones
    stacked = jnp.transpose(source, (1, 0, 2)).reshape(height, planes * width)
    solved = lax.linalg.tridiagonal_solve(lower, middle, upper, stacked)
    return jnp.transpose(solved.reshape(height, planes, width), (1, 0, 2))

def one_field(field, rate, stream_speed, wall_velocity):
    height = field.shape[1]
    streamwise = (45.0 * (jnp.roll(field, -1, 2) - jnp.roll(field, 1, 2)) - 9.0 * (jnp.roll(field, -2, 2) - jnp.roll(field, 2, 2)) + (jnp.roll(field, -3, 2) - jnp.roll(field, 3, 2))) / 60.0
    padded = jnp.pad(field, ((0, 0), (2, 2), (0, 0)))
    source = 0.5 * compact_near * (padded[:, 3:height + 3] - padded[:, 1:height + 1]) + 0.25 * compact_far * (padded[:, 4:height + 4] - padded[:, 0:height])
    unit = jnp.ones((), dtype=field.dtype)
    normal_slope = banded_solve(compact_alpha * unit, unit, source)
    tendency = -(stream_speed * streamwise + wall_velocity * normal_slope)
    smoothed = banded_solve(-rate, 1.0 + 2.0 * rate, 2.0 * field + time_step * tendency)
    return (tendency, smoothed - field)

def reference(fields, wall_velocity, diffusion):
    stream_speed = fields[0]

    def apply_field(pair):
        return one_field(pair[0], pair[1], stream_speed, wall_velocity)
    tendency, advanced = lax.map(apply_field, (fields, diffusion))
    return (tendency, advanced)
```

```python
import functools
import math

import jax
import jax.numpy as jnp
from jax import lax
from jax.experimental import pallas as pl
from jax.experimental.pallas import tpu as pltpu
from jax.sharding import PartitionSpec as P

time_step = 0.25
compact_alpha = 1.0 / 3.0
compact_near = 14.0 / 9.0
compact_far = 1.0 / 9.0
slope_ratio = (math.sqrt(1.0 - 4.0 * compact_alpha**2) - 1.0) / (2.0 * compact_alpha)
mix = 0.25 * compact_far / compact_alpha
rest = 0.5 * compact_near - mix
green = 1.0 / (1.0 + 2.0 * compact_alpha * slope_ratio)
kappa = rest * green * (slope_ratio - 1.0 / slope_ratio)
slope_gain = kappa * slope_ratio
slope_edge = -mix / slope_gain
tiny = 1.1754943508222875e-38
GROUP = 4
f32 = jnp.float32
MIB = 1 << 20


def params(mib):
    return pltpu.CompilerParams(vmem_limit_bytes=mib * MIB)


def lines(x):
    rows, cols = x.shape[-2:]
    y = x.reshape(-1, rows // 8, 8, cols // 128, 128)
    return jnp.swapaxes(y, 2, 3).reshape(-1, rows // 8, cols // 16, 128)


def unlines(y, shape):
    planes, tiles, wide, _ = y.shape
    y = y.reshape(planes, tiles, wide // 8, 8, 128)
    return jnp.swapaxes(y, 2, 3).reshape(shape)


def place():
    here = lax.axis_index("wall")
    return here, here == 0, here == lax.axis_size("wall") - 1


def edges_kernel(field_hbm, diffusion_hbm, field, sides, own, odd_out, even_out, coef, flag, rate, sems):
    planes, tiles = field.shape[0], field.shape[1]
    half = tiles // 2
    split = 4
    part = half // split
    copies = [pltpu.make_async_copy(field_hbm.at[p], field.at[p], sems.at[p]) for p in range(planes)]
    rates = pltpu.make_async_copy(diffusion_hbm, rate, sems.at[planes])
    rates.start()
    for copy in copies:
        copy.start()
    odd = place()[0] % 2 == 1

    def row(p, tile, r):
        return field[p, tile, pl.ds(r, 8, stride=8), :]

    rates.wait()
    longest = jnp.zeros((8, 128), f32)
    for k in range(rate.shape[0]):
        d = jnp.full((8, 128), rate[k])
        larger = 0.5 * (1.0 + 2.0 * d + jnp.sqrt(1.0 + 4.0 * d))
        ratio = d / larger
        log_ratio = jnp.log(ratio)
        weight = jnp.exp(8.0 * tiles * log_ratio)
        damp = 1.0 - ratio * ratio
        gain = time_step / larger
        for i, value in enumerate((ratio, gain, damp, weight, log_ratio, gain / damp)):
            coef[k, i] = value
        longest = jnp.maximum(longest, weight)
    flag[0] = (jnp.max(longest * longest) >= tiny).astype(jnp.int32)

    for p in range(planes):
        copies[p].wait()

        def step(t, carry, p=p):
            below, above = carry
            for r in range(8):
                below = [row(p, half + part * s + t, r) + slope_ratio * b for s, b in enumerate(below)]
                above = [row(p, part * s + part - 1 - t, 7 - r) + slope_ratio * a for s, a in enumerate(above)]
            return below, above

        zero = jnp.zeros((8, 128), f32)
        below, above = lax.fori_loop(0, part, step, ([zero] * split, [zero] * split))
        u, v = below[0], above[split - 1]
        jump = slope_ratio ** (8 * part)
        for s in range(1, split):
            u = below[s] + jump * u
            v = above[split - 1 - s] + jump * v
        top, bottom = row(p, tiles - 1, 7), row(p, 0, 0)
        for i, (a, b) in enumerate(((u, v), (top, bottom))):
            own[0, i, p] = a
            own[1, i, p] = b
            odd_out[i, p] = jnp.where(odd, a, b)
            even_out[i, p] = jnp.where(odd, b, a)
        for t in range(tiles):
            sides[0, p, t] = field[p, t, 0:8, :]
            sides[1, p, t] = field[p, t, 56:64, :]


def stencil():
    source = lax.broadcasted_iota(jnp.int32, (256, 256), 0) % 128
    target = lax.broadcasted_iota(jnp.int32, (256, 256), 1)
    offset = source - target % 128
    beyond = jnp.where(offset > 64, offset - 128, offset + 128)
    offset = jnp.where(target < 128, offset, beyond)
    size = jnp.abs(offset)
    value = jnp.where(size == 1, 45.0, jnp.where(size == 2, -9.0, jnp.where(size == 3, 1.0, 0.0)))
    return jnp.where(offset > 0, value, -value).astype(jnp.bfloat16)


def stream_kernel(field, sides, wall_hbm, out, wall, near, sem):
    planes, tiles = field.shape[0], field.shape[1]
    count = planes // 2
    copy = pltpu.make_async_copy(wall_hbm, wall, sem)
    copy.start()
    lane = lax.broadcasted_iota(jnp.int32, (8, 128), 1)
    matrix = stencil()
    group = GROUP

    def spread(x):
        high = x.astype(jnp.bfloat16)
        low = (x - high.astype(f32)).astype(jnp.bfloat16)
        return jnp.dot(jnp.concatenate([high, low], axis=1), matrix, preferred_element_type=f32)

    def outer(g, carry):
        p = g // 2
        side = g % 2
        x = sides[side, p].reshape(tiles * 8, 128)
        near[side, p] = spread(x)[:, 128:].reshape(tiles, 8, 128)
        return carry

    lax.fori_loop(0, 2 * planes, outer, 0)

    def body(g, carry):
        z = g // (tiles // group)
        first = (g % (tiles // group)) * group
        for k in range(count):
            p = k * 2 + z
            x = field[p, pl.ds(first, group)].reshape(group * 64, 128)
            both = spread(x)
            for t in range(group):
                tile = first + t
                part = [both[t * 64 + 8 * i : t * 64 + 8 * i + 8, 128:] for i in range(8)]
                part = [near[1, p, tile]] + part + [near[0, p, tile]]
                for i in range(8):
                    d = both[t * 64 + 8 * i : t * 64 + 8 * i + 8, :128]
                    d = d + jnp.where(lane < 64, part[i], part[i + 2])
                    speed = field[z, tile, 8 * i : 8 * i + 8, :] * (-1.0 / 60.0)
                    out[p, tile, 8 * i : 8 * i + 8, :] = speed * d
        return carry

    lax.fori_loop(0, 2 * tiles // group, body, 0)
    copy.wait()


def sweep_kernel(
    coef, field, stream, wall, own, odd_in, even_in, tend_hbm, adv, total, odd1, even1, odd2, even2, work, tend, sems
):
    planes, tiles = field.shape[0], field.shape[1]
    count = planes // 2
    ks = range(count)
    here, first, last_block = place()
    odd = here % 2 == 1
    pair = (here // 2) % 2 == 1
    image = mix / kappa

    def below(i, p):
        inner = jnp.where(odd, even_in[i, p], odd_in[i, p])
        edge = slope_ratio * own[1, 0, p] - image * own[1, 1, p] if i == 0 else jnp.zeros((8, 128), f32)
        return jnp.where(first, edge, inner)

    def above(i, p):
        inner = jnp.where(odd, odd_in[i, p], even_in[i, p])
        edge = slope_ratio * own[0, 0, p] - image * own[0, 1, p] if i == 0 else jnp.zeros((8, 128), f32)
        return jnp.where(last_block, edge, inner)

    def row(ref, p, tile, r):
        return ref[p, tile, pl.ds(r, 8, stride=8), :]

    ratio = [coef[k, 0] for k in ks]
    copies = []
    for z in range(2):
        at = [2 * k + z for k in ks]

        def rise(t, u):
            for r in range(8):
                for k in ks:
                    work[k, t, 8 * r : 8 * r + 8, :] = u[k]
                u = [row(field, at[k], t, r) + slope_ratio * u[k] for k in ks]
            return u

        lax.fori_loop(0, tiles, rise, [below(0, at[k]) for k in ks])

        ghost = [below(1, at[k]) for k in ks]

        def fall(i, carry):
            v, ahead, here, total = carry
            t = tiles - 1 - i
            for r in range(7, -1, -1):
                speed = row(wall, z, t, r) * (-slope_gain)
                if r > 0:
                    last = [row(field, at[k], t, r - 1) for k in ks]
                else:
                    before = jnp.maximum(t - 1, 0)
                    last = [jnp.where(t == 0, ghost[k], row(field, at[k], before, 7)) for k in ks]
                slope = [
                    (work[k, t, 8 * r : 8 * r + 8, :] - v[k]) + slope_edge * (last[k] - ahead[k]) for k in ks
                ]
                rate = [row(stream, at[k], t, r) + speed * slope[k] for k in ks]
                for k in ks:
                    tend[at[k], t, pl.ds(r, 8, stride=8), :] = rate[k]
                total = [(rate[k] + 8.0 * here[k]) + ratio[k] * total[k] for k in ks]
                for k in ks:
                    work[k, t, 8 * r : 8 * r + 8, :] = total[k]
                v = [here[k] + slope_ratio * v[k] for k in ks]
                ahead, here = here, last
            return v, ahead, here, total

        zero = jnp.zeros((8, 128), f32)
        start = (
            [above(0, at[k]) for k in ks],
            [above(1, at[k]) for k in ks],
            [row(field, at[k], tiles - 1, 7) for k in ks],
            [zero] * count,
        )
        bottom = lax.fori_loop(0, tiles, fall, start)[3]
        for k in ks:
            copy = pltpu.make_async_copy(tend.at[at[k]], tend_hbm.at[at[k]], sems.at[at[k]])
            copy.start()
            copies.append(copy)
        gain = [coef[k, 1] for k in ks]

        def settle(t, q):
            for r in range(8):
                q = [work[k, t, 8 * r : 8 * r + 8, :] + ratio[k] * q[k] for k in ks]
                for k in ks:
                    adv[at[k], t, pl.ds(r, 8, stride=8), :] = gain[k] * q[k] - row(field, at[k], t, r)
            return q

        top = lax.fori_loop(0, tiles, settle, [zero] * count)
        for k in ks:
            p = at[k]
            weight = coef[k, 3]
            up = coef[k, 2] * top[k] + weight * ratio[k] * bottom[k]
            down = bottom[k]
            total[0, p] = up
            total[1, p] = down
            send_up = jnp.where(first, up - weight * ratio[k] * down, up)
            send_down = jnp.where(last_block, down - weight * ratio[k] * up, down)
            odd1[p] = jnp.where(odd, send_up, send_down)
            even1[p] = jnp.where(odd, send_down, send_up)
            odd2[p] = jnp.where(pair, send_up, send_down)
            even2[p] = jnp.where(pair, send_down, send_up)
    for copy in copies:
        copy.wait()


def two_blocks(p, coef, total, odd1, even1, odd2, even2):
    here, first, last_block = place()
    odd = here % 2 == 1
    pair = (here // 2) % 2 == 1
    ratio, weight = coef[p // 2, 0], coef[p // 2, 3]
    low = jnp.where(odd, even1[p], odd1[p]) + weight * jnp.where(pair, even2[p], odd2[p])
    high = jnp.where(odd, odd1[p], even1[p]) + weight * jnp.where(pair, odd2[p], even2[p])
    end_low = -ratio * (total[1, p] + weight * high)
    end_high = -ratio * (total[0, p] + weight * low)
    return jnp.where(first, end_low, low), jnp.where(last_block, end_high, high)


def finish_kernel(coef, partial, total, odd1, even1, odd2, even2, out_hbm, out, sems):
    planes, tiles = partial.shape[0], partial.shape[1]
    line = lax.broadcasted_iota(jnp.int32, (8, 128), 0)
    copies = []
    for p in range(planes):
        k = p // 2
        ratio, log_ratio, scale = coef[k, 0], coef[k, 4], coef[k, 5]
        low, high = two_blocks(p, coef, total, odd1, even1, odd2, even2)
        low = scale * (ratio * total[1, p] + low)
        high = scale * high
        a = [jnp.broadcast_to(low[i : i + 1, :], (8, 128)) for i in range(8)]
        b = [jnp.broadcast_to(high[i : i + 1, :], (8, 128)) for i in range(8)]

        def body(t, carry, p=p, log_ratio=log_ratio, a=a, b=b):
            for s in range(2):
                tile = 2 * t + s
                at = (line + 8 * tile).astype(f32)
                fade = jnp.exp(log_ratio * (at + 1.0))
                grow = jnp.exp(log_ratio * (8.0 * tiles - at))
                for i in range(8):
                    piece = partial[p, tile, 8 * i : 8 * i + 8, :]
                    out[p, tile, 8 * i : 8 * i + 8, :] = piece + (fade * a[i] + grow * b[i])
            return carry

        lax.fori_loop(0, tiles // 2, body, 0)
        copy = pltpu.make_async_copy(out.at[p], out_hbm.at[p], sems.at[p])
        copy.start()
        copies.append(copy)
    for copy in copies:
        copy.wait()


def chain_kernel(coef, total, from_below, from_above, low_in, high_in, low_out, high_out, up_out, down_out):
    _, first, last_block = place()
    for p in range(total.shape[1]):
        ratio, weight = coef[p // 2, 0], coef[p // 2, 3]
        up, down = total[0, p], total[1, p]
        low = jnp.where(first, -ratio * (down + weight * high_in[p]), from_below[p])
        high = jnp.where(last_block, -ratio * (up + weight * low_in[p]), from_above[p])
        low_out[p] = low
        high_out[p] = high
        up_out[p] = up + weight * low
        down_out[p] = down + weight * high


def clear_kernel(*refs):
    for ref in refs:
        ref[...] = jnp.zeros(ref.shape, f32)


def chain_end_kernel(advanced, coef, total, odd1, even1, odd2, even2, low, high, out):
    planes, tiles = advanced.shape[0], advanced.shape[1]
    line = lax.broadcasted_iota(jnp.int32, (8, 128), 0)
    for p in range(planes):
        log_ratio, scale = coef[p // 2, 4], coef[p // 2, 5]
        near_low, near_high = two_blocks(p, coef, total, odd1, even1, odd2, even2)
        more_low = scale * (low[p] - near_low)
        more_high = scale * (high[p] - near_high)

        def body(tile, carry, p=p, log_ratio=log_ratio, more_low=more_low, more_high=more_high):
            at = (line + 8 * tile).astype(f32)
            fade = jnp.exp(log_ratio * (at + 1.0))
            grow = jnp.exp(log_ratio * (8.0 * tiles - at))
            for i in range(8):
                low_row = jnp.broadcast_to(more_low[i : i + 1, :], (8, 128))
                high_row = jnp.broadcast_to(more_high[i : i + 1, :], (8, 128))
                piece = advanced[p, tile, 8 * i : 8 * i + 8, :]
                out[p, tile, 8 * i : 8 * i + 8, :] = piece + (fade * low_row + grow * high_row)
            return carry

        lax.fori_loop(0, tiles, body, 0)


VMEM = pl.BlockSpec(memory_space=pltpu.VMEM)
SMEM = pl.BlockSpec(memory_space=pltpu.SMEM)
ANY = pl.BlockSpec(memory_space=pl.ANY)


def pairs(count, by, odd):
    found = []
    for a in range(count - by):
        if (a // by) % 2 == odd:
            found += [(a, a + by), (a + by, a)]
    return found


def exchange(odd, even, by):
    count = lax.axis_size("wall")
    return (
        lax.ppermute(odd, "wall", pairs(count, by, 1)),
        lax.ppermute(even, "wall", pairs(count, by, 0)),
    )


def whole_chain(advanced, coef, total, *arrived):
    count = lax.axis_size("wall")
    rise = [(i, i + 1) for i in range(count - 1)]
    fall = [(i + 1, i) for i in range(count - 1)]
    rows = jax.ShapeDtypeStruct(total.shape[1:], f32)

    def step(_, carry):
        low, high, up, down = carry
        return list(pl.pallas_call(
            chain_kernel,
            in_specs=[VMEM] * 6,
            out_specs=[VMEM] * 4,
            out_shape=[rows] * 4,
            compiler_params=params(2),
            name="chain",
        )(coef, total, lax.ppermute(up, "wall", rise), lax.ppermute(down, "wall", fall), low, high))

    start = list(pl.pallas_call(
        clear_kernel,
        out_specs=[VMEM] * 4,
        out_shape=[rows] * 4,
        compiler_params=params(2),
        name="chain_start",
    )())
    low, high, _, _ = lax.fori_loop(0, 2 * count, step, start)
    return pl.pallas_call(
        chain_end_kernel,
        in_specs=[VMEM] * 9,
        out_specs=VMEM,
        out_shape=jax.ShapeDtypeStruct(advanced.shape, f32),
        compiler_params=params(24),
        name="chain_end",
    )(advanced, coef, total, *arrived, low, high)


def on_device(fields, wall_velocity, diffusion):
    count, depth, height, width = fields.shape
    planes, tiles = count * depth, height // 8
    wide = width // 16
    shape = jax.ShapeDtypeStruct
    full = (planes, tiles, wide, 128)
    resident = pltpu.VMEM(full, f32)
    rows = shape((planes, 8, 128), f32)
    ends = shape((2, planes, 8, 128), f32)
    in_hbm = functools.partial(pltpu.with_memory_space_constraint, memory_space=pltpu.HBM)

    field, sides, own, odd, even, coef, flag = pl.pallas_call(
        edges_kernel,
        in_specs=[ANY, ANY],
        out_specs=[VMEM] * 6 + [SMEM],
        out_shape=[
            resident,
            shape((2, planes, tiles, 8, 128), f32),
            pltpu.VMEM((2, 2, planes, 8, 128), f32),
            ends,
            ends,
            pltpu.VMEM((count, 6, 8, 128), f32),
            shape((1,), jnp.int32),
        ],
        scratch_shapes=[pltpu.SMEM((count,), f32), pltpu.SemaphoreType.DMA((planes + 1,))],
        compiler_params=params(4),
        name="edges",
    )(in_hbm(lines(fields)), in_hbm(diffusion))
    sides = lax.ppermute(sides, "stream", [(0, 1), (1, 0)])
    odd, even = exchange(odd, even, 1)

    stream, wall = pl.pallas_call(
        stream_kernel,
        in_specs=[VMEM, VMEM, ANY],
        out_specs=[VMEM] * 2,
        out_shape=[resident, pltpu.VMEM((depth, tiles, wide, 128), f32)],
        scratch_shapes=[pltpu.VMEM((2, planes, tiles, 8, 128), f32), pltpu.SemaphoreType.DMA],
        compiler_params=params(8),
        cost_estimate=pl.CostEstimate(flops=4_000_000_000, transcendentals=0, bytes_accessed=0),
        name="streamwise",
    )(field, sides, in_hbm(lines(wall_velocity)))

    tendency, partial, total, *sent = pl.pallas_call(
        sweep_kernel,
        in_specs=[VMEM] * 7,
        out_specs=[ANY] + [VMEM] * 6,
        out_shape=[shape(full, f32), resident, pltpu.VMEM((2, planes, 8, 128), f32)] + [rows] * 4,
        scratch_shapes=[
            pltpu.VMEM((count, tiles, wide, 128), f32),
            pltpu.VMEM(full, f32),
            pltpu.SemaphoreType.DMA((planes,)),
        ],
        compiler_params=params(14),
        name="sweeps",
    )(coef, field, stream, wall, own, odd, even)

    odd1, even1, odd2, even2 = sent
    far = exchange(odd2, even2, 2)
    near = exchange(odd1, even1, 1)
    arrived = [*near, *far]

    advanced = pl.pallas_call(
        finish_kernel,
        in_specs=[VMEM] * 7,
        out_specs=ANY,
        out_shape=shape(full, f32),
        scratch_shapes=[pltpu.VMEM(full, f32), pltpu.SemaphoreType.DMA((planes,))],
        compiler_params=params(10),
        name="finish",
    )(coef, partial, total, *arrived)
    advanced = lax.cond(flag[0] != 0, whole_chain, lambda x, *_: x, advanced, coef, total, *arrived)
    return unlines(tendency, fields.shape), unlines(advanced, fields.shape)


def solution(mesh):
    tall = P(None, None, "wall", "stream")
    return jax.shard_map(
        on_device,
        mesh=mesh,
        in_specs=(tall, P(None, "wall", "stream"), P()),
        out_specs=(tall, tall),
        check_vma=False,
    )
```

```python
import functools
import math

import jax
import jax.numpy as jnp
from jax import lax
from jax.experimental import pallas as pl
from jax.experimental.pallas import tpu as pltpu
from jax.sharding import PartitionSpec as P

time_step = 0.25
compact_alpha = 1.0 / 3.0
compact_near = 14.0 / 9.0
compact_far = 1.0 / 9.0
slope_ratio = (math.sqrt(1.0 - 4.0 * compact_alpha**2) - 1.0) / (2.0 * compact_alpha)
mix = 0.25 * compact_far / compact_alpha
rest = 0.5 * compact_near - mix
green = 1.0 / (1.0 + 2.0 * compact_alpha * slope_ratio)
kappa = rest * green * (slope_ratio - 1.0 / slope_ratio)
slope_gain = kappa * slope_ratio
slope_edge = -mix / slope_gain
tiny = 1.1754943508222875e-38
SPLIT = 6
f32 = jnp.float32
MIB = 1 << 20


def params(mib):
    return pltpu.CompilerParams(vmem_limit_bytes=mib * MIB)


def lines(x):
    rows, cols = x.shape[-2:]
    y = x.reshape(-1, rows // 8, 8, cols // 128, 128)
    return jnp.swapaxes(y, 2, 3)[:, :, :, :, None, :]


def unlines(y, shape):
    return jnp.swapaxes(y[:, :, :, :, 0, :], 2, 3).reshape(shape)


def load_rows(hbm, rows, sems, p):
    return [
        pltpu.make_async_copy(hbm.at[p, :, :, r, 0], rows.at[p, :, r], sems.at[p, r]) for r in range(8)
    ]


def store_rows(rows, hbm, sems, p):
    return [
        pltpu.make_async_copy(rows.at[p, :, r], hbm.at[p, :, :, r, 0], sems.at[p, r]) for r in range(8)
    ]


def place():
    here = lax.axis_index("wall")
    return here, here == 0, here == lax.axis_size("wall") - 1


def edges_kernel(field_hbm, diffusion_hbm, field, sides, own, odd_out, even_out, coef, fading, flag, rate, sems, sem):
    planes, tiles = field.shape[0], field.shape[1]
    half = tiles // 2
    split = SPLIT
    part = half // split
    rates = pltpu.make_async_copy(diffusion_hbm, rate, sem)
    rates.start()
    copies = [load_rows(field_hbm, field, sems, p) for p in range(planes)]
    for copy in sum(copies, []):
        copy.start()
    odd = place()[0] % 2 == 1

    def coefficients():
        rates.wait()
        longest = jnp.zeros((8, 128), f32)
        for k in range(rate.shape[0]):
            d = jnp.full((8, 128), rate[k])
            larger = 0.5 * (1.0 + 2.0 * d + jnp.sqrt(1.0 + 4.0 * d))
            ratio = d / larger
            log_ratio = jnp.log(ratio)
            weight = jnp.exp(8.0 * tiles * log_ratio)
            damp = 1.0 - ratio * ratio
            gain = time_step / larger
            for i, value in enumerate((ratio, gain, damp, weight, log_ratio, gain / damp)):
                coef[k, i] = value
            longest = jnp.maximum(longest, weight)
            line = lax.broadcasted_iota(jnp.int32, (8, 128), 0).astype(f32) + 1.0
            for tile in range(tiles):
                fading[k, tile] = jnp.exp(log_ratio * (line + 8.0 * tile))
        flag[0] = (jnp.max(longest * longest) >= tiny).astype(jnp.int32)

    for p in range(planes):
        for copy in copies[p]:
            copy.wait()
        if p == planes // 2:
            coefficients()

        def step(t, carry, p=p):
            below, above = carry
            for r in range(8):
                below = [field[p, half + part * s + t, r] + slope_ratio * b for s, b in enumerate(below)]
                above = [field[p, part * s + part - 1 - t, 7 - r] + slope_ratio * a for s, a in enumerate(above)]
            return below, above

        zero = jnp.zeros((8, 128), f32)
        below, above = lax.fori_loop(0, part, step, ([zero] * split, [zero] * split))
        u, v = below[0], above[split - 1]
        jump = slope_ratio ** (8 * part)
        for s in range(1, split):
            u = below[s] + jump * u
            v = above[split - 1 - s] + jump * v
        top, bottom = field[p, tiles - 1, 7], field[p, 0, 0]
        for i, (a, b) in enumerate(((u, v), (top, bottom))):
            own[0, i, p] = a
            own[1, i, p] = b
            odd_out[i, p] = jnp.where(odd, a, b)
            even_out[i, p] = jnp.where(odd, b, a)
        flat = field.at[p].reshape(tiles * 64, 128)
        for t in range(tiles):
            sides[0, p, t] = flat[pl.ds(64 * t, 8, stride=8), :]
            sides[1, p, t] = flat[pl.ds(64 * t + 7, 8, stride=8), :]


def stencil():
    source = lax.broadcasted_iota(jnp.int32, (256, 256), 0) % 128
    target = lax.broadcasted_iota(jnp.int32, (256, 256), 1)
    offset = source - target % 128
    beyond = jnp.where(offset > 64, offset - 128, offset + 128)
    offset = jnp.where(target < 128, offset, beyond)
    size = jnp.abs(offset)
    value = jnp.where(size == 1, 45.0, jnp.where(size == 2, -9.0, jnp.where(size == 3, 1.0, 0.0)))
    return jnp.where(offset > 0, value, -value).astype(jnp.bfloat16)


def stream_kernel(field, sides, wall_hbm, out, wall, near, sems):
    planes, tiles = field.shape[0], field.shape[1]
    copies = sum([load_rows(wall_hbm, wall, sems, z) for z in range(wall.shape[0])], [])
    for copy in copies:
        copy.start()
    lane = lax.broadcasted_iota(jnp.int32, (8, 128), 1)
    piece = lax.broadcasted_iota(jnp.int32, (8, 128), 0)
    left = lane < 64
    outer = ((piece == 0) & left) | ((piece == 7) & (lane >= 64))
    matrix = stencil()

    def spread(x, columns):
        high = x.astype(jnp.bfloat16)
        low = (x - high.astype(f32)).astype(jnp.bfloat16)
        return jnp.dot(jnp.concatenate([high, low], axis=1), columns, preferred_element_type=f32)

    before = spread(sides[1].reshape(planes * tiles * 8, 128), matrix[:, 128:])
    after = spread(sides[0].reshape(planes * tiles * 8, 128), matrix[:, 128:])
    first = lax.broadcasted_iota(jnp.int32, before.shape, 1) < 64
    near[...] = jnp.where(first, before, after).reshape(planes, tiles, 8, 128)

    def body(p, carry):
        both = spread(field[p].reshape(tiles * 64, 128), matrix)
        for tile in range(tiles):
            for r in range(8):
                at = tile * 64 + 8 * r
                part = both[at : at + 8, 128:]
                part = jnp.where(left, pltpu.roll(part, 1, 0), pltpu.roll(part, 7, 0))
                part = jnp.where(outer, jnp.broadcast_to(near[p, tile, r : r + 1, :], (8, 128)), part)
                speed = field[p % 2, tile, r] * (-1.0 / 60.0)
                out[p, tile, r] = speed * (both[at : at + 8, :128] + part)
        return carry

    lax.fori_loop(0, planes, body, 0)
    for copy in copies:
        copy.wait()


def sweep_kernel(
    coef, field, stream, wall, own, odd_in, even_in, tend_hbm, adv, total, odd1, even1, odd2, even2, work, tend, sems
):
    planes, tiles = field.shape[0], field.shape[1]
    count = planes // 2
    ks = range(count)
    here, first, last_block = place()
    odd = here % 2 == 1
    pair = (here // 2) % 2 == 1
    image = mix / kappa

    def below(i, p):
        inner = jnp.where(odd, even_in[i, p], odd_in[i, p])
        edge = slope_ratio * own[1, 0, p] - image * own[1, 1, p] if i == 0 else jnp.zeros((8, 128), f32)
        return jnp.where(first, edge, inner)

    def above(i, p):
        inner = jnp.where(odd, odd_in[i, p], even_in[i, p])
        edge = slope_ratio * own[0, 0, p] - image * own[0, 1, p] if i == 0 else jnp.zeros((8, 128), f32)
        return jnp.where(last_block, edge, inner)

    every = range(planes)
    ratio = [coef[k, 0] for k in ks]
    copies = []
    zero = jnp.zeros((8, 128), f32)

    def rise(t, u):
        for r in range(8):
            for p in every:
                work[p, t, r] = u[p]
            u = [field[p, t, r] + slope_ratio * u[p] for p in every]
        return u

    lax.fori_loop(0, tiles, rise, [below(0, p) for p in every])

    bottom = {}
    for z in range(2):
        at = [2 * k + z for k in ks]
        ghost = [below(1, at[k]) for k in ks]

        def fall(i, carry, z=z, at=at, ghost=ghost):
            v, ahead, here, total = carry
            t = tiles - 1 - i
            for r in range(7, -1, -1):
                speed = wall[z, t, r] * (-slope_gain)
                if r > 0:
                    last = [field[at[k], t, r - 1] for k in ks]
                else:
                    before = jnp.maximum(t - 1, 0)
                    last = [jnp.where(t == 0, ghost[k], field[at[k], before, 7]) for k in ks]
                slope = [
                    (work[at[k], t, r] - v[k]) + slope_edge * (last[k] - ahead[k]) for k in ks
                ]
                rate = [stream[at[k], t, r] + speed * slope[k] for k in ks]
                for k in ks:
                    tend[at[k], t, r] = rate[k]
                total = [(rate[k] + 8.0 * here[k]) + ratio[k] * total[k] for k in ks]
                for k in ks:
                    work[at[k], t, r] = total[k]
                v = [here[k] + slope_ratio * v[k] for k in ks]
                ahead, here = here, last
            return v, ahead, here, total

        start = (
            [above(0, at[k]) for k in ks],
            [above(1, at[k]) for k in ks],
            [field[at[k], tiles - 1, 7] for k in ks],
            [zero] * count,
        )
        lowest = lax.fori_loop(0, tiles, fall, start)[3]
        for k in ks:
            bottom[at[k]] = lowest[k]
            for copy in store_rows(tend, tend_hbm, sems, at[k]):
                copy.start()
                copies.append(copy)
    gain = [coef[k, 1] for k in ks]

    def settle(t, q):
        for r in range(8):
            q = [work[p, t, r] + ratio[p // 2] * q[p] for p in every]
            for p in every:
                adv[p, t, r] = gain[p // 2] * q[p] - field[p, t, r]
        return q

    top = lax.fori_loop(0, tiles, settle, [zero] * planes)
    for p in every:
        weight, step = coef[p // 2, 3], ratio[p // 2]
        up = coef[p // 2, 2] * top[p] + weight * step * bottom[p]
        down = bottom[p]
        total[0, p] = up
        total[1, p] = down
        send_up = jnp.where(first, up - weight * step * down, up)
        send_down = jnp.where(last_block, down - weight * step * up, down)
        odd1[p] = jnp.where(odd, send_up, send_down)
        even1[p] = jnp.where(odd, send_down, send_up)
        odd2[p] = jnp.where(pair, send_up, send_down)
        even2[p] = jnp.where(pair, send_down, send_up)
    for copy in copies:
        copy.wait()


def two_blocks(p, coef, total, odd1, even1, odd2, even2):
    here, first, last_block = place()
    odd = here % 2 == 1
    pair = (here // 2) % 2 == 1
    ratio, weight = coef[p // 2, 0], coef[p // 2, 3]
    low = jnp.where(odd, even1[p], odd1[p]) + weight * jnp.where(pair, even2[p], odd2[p])
    high = jnp.where(odd, odd1[p], even1[p]) + weight * jnp.where(pair, odd2[p], even2[p])
    end_low = -ratio * (total[1, p] + weight * high)
    end_high = -ratio * (total[0, p] + weight * low)
    return jnp.where(first, end_low, low), jnp.where(last_block, end_high, high)


def add_ends(k, lows, highs, fading, source, target):
    tiles = source.shape[1]

    def body(t, carry):
        for r in range(8):
            fade = jnp.broadcast_to(fading[k, t, r : r + 1, :], (8, 128))
            grow = jnp.broadcast_to(fading[k, tiles - 1 - t, 7 - r : 8 - r, :], (8, 128))
            for p, low, high in zip((2 * k, 2 * k + 1), lows, highs):
                target[p, t, r] = source[p, t, r] + (fade * low + grow * high)
        return carry

    lax.fori_loop(0, tiles, body, 0)


def finish_kernel(coef, fading, partial, total, odd1, even1, odd2, even2, out_hbm, out, sems):
    copies = []
    for k in range(coef.shape[0]):
        ratio, scale = coef[k, 0], coef[k, 5]
        lows, highs = [], []
        for p in (2 * k, 2 * k + 1):
            low, high = two_blocks(p, coef, total, odd1, even1, odd2, even2)
            lows.append(scale * (ratio * total[1, p] + low))
            highs.append(scale * high)
        add_ends(k, lows, highs, fading, partial, out)
        for p in (2 * k, 2 * k + 1):
            for copy in store_rows(out, out_hbm, sems, p):
                copy.start()
                copies.append(copy)
    for copy in copies:
        copy.wait()


def chain_kernel(coef, total, from_below, from_above, low_in, high_in, low_out, high_out, up_out, down_out):
    _, first, last_block = place()
    for p in range(total.shape[1]):
        ratio, weight = coef[p // 2, 0], coef[p // 2, 3]
        up, down = total[0, p], total[1, p]
        low = jnp.where(first, -ratio * (down + weight * high_in[p]), from_below[p])
        high = jnp.where(last_block, -ratio * (up + weight * low_in[p]), from_above[p])
        low_out[p] = low
        high_out[p] = high
        up_out[p] = up + weight * low
        down_out[p] = down + weight * high


def clear_kernel(*refs):
    for ref in refs:
        ref[...] = jnp.zeros(ref.shape, f32)


def chain_end_kernel(
    advanced_hbm, coef, fading, total, odd1, even1, odd2, even2, low, high, out_hbm, before, after, loads, stores
):
    for k in range(coef.shape[0]):
        pair = (2 * k, 2 * k + 1)
        scale = coef[k, 5]
        lows, highs = [], []
        for p in pair:
            near_low, near_high = two_blocks(p, coef, total, odd1, even1, odd2, even2)
            lows.append(scale * (low[p] - near_low))
            highs.append(scale * (high[p] - near_high))
        copies = sum([load_rows(advanced_hbm, before, loads, p) for p in pair], [])
        for copy in copies:
            copy.start()
        for copy in copies:
            copy.wait()
        add_ends(k, lows, highs, fading, before, after)
        copies = sum([store_rows(after, out_hbm, stores, p) for p in pair], [])
        for copy in copies:
            copy.start()
        for copy in copies:
            copy.wait()


VMEM = pl.BlockSpec(memory_space=pltpu.VMEM)
SMEM = pl.BlockSpec(memory_space=pltpu.SMEM)
ANY = pl.BlockSpec(memory_space=pl.ANY)


def pairs(count, by, odd):
    found = []
    for a in range(count - by):
        if (a // by) % 2 == odd:
            found += [(a, a + by), (a + by, a)]
    return found


def row_shape(shape):
    planes, tiles = shape[:2]
    return (planes, tiles, 8, 8, 128)


def exchange(odd, even, by):
    count = lax.axis_size("wall")
    return (
        lax.ppermute(odd, "wall", pairs(count, by, 1)),
        lax.ppermute(even, "wall", pairs(count, by, 0)),
    )


def whole_chain(advanced, coef, fading, total, *arrived):
    count = lax.axis_size("wall")
    rise = [(i, i + 1) for i in range(count - 1)]
    fall = [(i + 1, i) for i in range(count - 1)]
    rows = jax.ShapeDtypeStruct(total.shape[1:], f32)
    planes = advanced.shape[0]

    def step(_, carry):
        low, high, up, down = carry
        return list(pl.pallas_call(
            chain_kernel,
            in_specs=[VMEM] * 6,
            out_specs=[VMEM] * 4,
            out_shape=[rows] * 4,
            compiler_params=params(2),
            name="chain",
        )(coef, total, lax.ppermute(up, "wall", rise), lax.ppermute(down, "wall", fall), low, high))

    start = list(pl.pallas_call(
        clear_kernel,
        out_specs=[VMEM] * 4,
        out_shape=[rows] * 4,
        compiler_params=params(2),
        name="chain_start",
    )())
    low, high, _, _ = lax.fori_loop(0, 2 * count, step, start)
    return pl.pallas_call(
        chain_end_kernel,
        in_specs=[ANY] + [VMEM] * 9,
        out_specs=ANY,
        out_shape=jax.ShapeDtypeStruct(advanced.shape, f32),
        scratch_shapes=[pltpu.VMEM(row_shape(advanced.shape), f32)] * 2 + [pltpu.SemaphoreType.DMA((planes, 8))] * 2,
        compiler_params=params(18),
        name="chain_end",
    )(advanced, coef, fading, total, *arrived, low, high)


def on_device(fields, wall_velocity, diffusion):
    count, depth, height, width = fields.shape
    planes, tiles = count * depth, height // 8
    shape = jax.ShapeDtypeStruct
    source, wall_source = lines(fields), lines(wall_velocity)
    full = row_shape(source.shape)
    resident = pltpu.VMEM(full, f32)
    rows = shape((planes, 8, 128), f32)
    ends = shape((2, planes, 8, 128), f32)
    in_hbm = functools.partial(pltpu.with_memory_space_constraint, memory_space=pltpu.HBM)
    plane_sems = pltpu.SemaphoreType.DMA((planes, 8))

    field, sides, own, odd, even, coef, fading, flag = pl.pallas_call(
        edges_kernel,
        in_specs=[ANY, ANY],
        out_specs=[VMEM] * 7 + [SMEM],
        out_shape=[
            resident,
            shape((2, planes, tiles, 8, 128), f32),
            pltpu.VMEM((2, 2, planes, 8, 128), f32),
            ends,
            ends,
            pltpu.VMEM((count, 6, 8, 128), f32),
            pltpu.VMEM((count, tiles, 8, 128), f32),
            shape((1,), jnp.int32),
        ],
        scratch_shapes=[pltpu.SMEM((count,), f32), plane_sems, pltpu.SemaphoreType.DMA],
        compiler_params=params(4),
        name="edges",
    )(in_hbm(source), in_hbm(diffusion))
    sides = lax.ppermute(sides, "stream", [(0, 1), (1, 0)])
    odd, even = exchange(odd, even, 1)

    stream, wall = pl.pallas_call(
        stream_kernel,
        in_specs=[VMEM, VMEM, ANY],
        out_specs=[VMEM] * 2,
        out_shape=[resident, pltpu.VMEM(row_shape(wall_source.shape), f32)],
        scratch_shapes=[pltpu.VMEM((planes, tiles, 8, 128), f32), pltpu.SemaphoreType.DMA((depth, 8))],
        compiler_params=params(12),
        cost_estimate=pl.CostEstimate(flops=4_000_000_000, transcendentals=0, bytes_accessed=0),
        name="streamwise",
    )(field, sides, in_hbm(wall_source))

    tendency, partial, total, *sent = pl.pallas_call(
        sweep_kernel,
        in_specs=[VMEM] * 7,
        out_specs=[ANY] + [VMEM] * 6,
        out_shape=[shape(source.shape, f32), resident, pltpu.VMEM((2, planes, 8, 128), f32)] + [rows] * 4,
        scratch_shapes=[pltpu.VMEM(full, f32), pltpu.VMEM(full, f32), plane_sems],
        compiler_params=params(18),
        name="sweeps",
    )(coef, field, stream, wall, own, odd, even)

    odd1, even1, odd2, even2 = sent
    far = exchange(odd2, even2, 2)
    near = exchange(odd1, even1, 1)
    arrived = [*near, *far]

    advanced = pl.pallas_call(
        finish_kernel,
        in_specs=[VMEM] * 8,
        out_specs=ANY,
        out_shape=shape(source.shape, f32),
        scratch_shapes=[pltpu.VMEM(full, f32), plane_sems],
        compiler_params=params(10),
        name="finish",
    )(coef, fading, partial, total, *arrived)
    advanced = lax.cond(flag[0] != 0, whole_chain, lambda x, *_: x, advanced, coef, fading, total, *arrived)
    return unlines(tendency, fields.shape), unlines(advanced, fields.shape)


def solution(mesh):
    tall = P(None, None, "wall", "stream")
    return jax.shard_map(
        on_device,
        mesh=mesh,
        in_specs=(tall, P(None, "wall", "stream"), P()),
        out_specs=(tall, tall),
        check_vma=False,
    )
```

```python
import functools
import math

import jax
import jax.numpy as jnp
from jax import lax
from jax.experimental import pallas as pl
from jax.experimental.pallas import tpu as pltpu
from jax.sharding import PartitionSpec as P

time_step = 0.25
compact_alpha = 1.0 / 3.0
compact_near = 14.0 / 9.0
compact_far = 1.0 / 9.0
slope_ratio = (math.sqrt(1.0 - 4.0 * compact_alpha**2) - 1.0) / (2.0 * compact_alpha)
mix = 0.25 * compact_far / compact_alpha
rest = 0.5 * compact_near - mix
green = 1.0 / (1.0 + 2.0 * compact_alpha * slope_ratio)
kappa = rest * green * (slope_ratio - 1.0 / slope_ratio)
slope_gain = kappa * slope_ratio
slope_edge = -mix / slope_gain
tiny = 1.1754943508222875e-38
SPLIT = 6
TOGETHER = 2
f32 = jnp.float32
MIB = 1 << 20


def params(mib):
    return pltpu.CompilerParams(vmem_limit_bytes=mib * MIB)


def lines(x):
    rows, cols = x.shape[-2:]
    y = x.reshape(-1, rows // 8, 8, cols // 128, 128)
    return jnp.swapaxes(y, 2, 3)[:, :, :, :, None, :]


def unlines(y, shape):
    return jnp.swapaxes(y[:, :, :, :, 0, :], 2, 3).reshape(shape)


def load_rows(hbm, rows, sems, p):
    return [
        pltpu.make_async_copy(hbm.at[p, :, :, r, 0], rows.at[p, :, r], sems.at[p, r]) for r in range(8)
    ]


def store_rows(rows, hbm, sems, p):
    return [
        pltpu.make_async_copy(rows.at[p, :, r], hbm.at[p, :, :, r, 0], sems.at[p, r]) for r in range(8)
    ]


def place():
    here = lax.axis_index("wall")
    return here, here == 0, here == lax.axis_size("wall") - 1


def edges_kernel(field_hbm, diffusion_hbm, field, sides, own, odd_out, even_out, coef, fading, flag, rate, sems, sem):
    planes, tiles = field.shape[0], field.shape[1]
    half = tiles // 2
    split = SPLIT
    part = half // split
    rates = pltpu.make_async_copy(diffusion_hbm, rate, sem)
    rates.start()
    copies = [load_rows(field_hbm, field, sems, p) for p in range(planes)]
    for copy in sum(copies, []):
        copy.start()
    odd = place()[0] % 2 == 1

    def coefficients():
        rates.wait()
        longest = jnp.zeros((8, 128), f32)
        for k in range(rate.shape[0]):
            d = jnp.full((8, 128), rate[k])
            larger = 0.5 * (1.0 + 2.0 * d + jnp.sqrt(1.0 + 4.0 * d))
            ratio = d / larger
            log_ratio = jnp.log(ratio)
            weight = jnp.exp(8.0 * tiles * log_ratio)
            damp = 1.0 - ratio * ratio
            gain = time_step / larger
            for i, value in enumerate((ratio, gain, damp, weight, log_ratio, gain / damp)):
                coef[k, i] = value
            longest = jnp.maximum(longest, weight)
            line = lax.broadcasted_iota(jnp.int32, (8, 128), 0).astype(f32) + 1.0
            for tile in range(tiles):
                fading[k, tile] = jnp.exp(log_ratio * (line + 8.0 * tile))
        flag[0] = (jnp.max(longest * longest) >= tiny).astype(jnp.int32)

    for p in range(planes):
        for copy in copies[p]:
            copy.wait()
        if p == planes // 2:
            coefficients()

        def step(t, carry, p=p):
            below, above = carry
            for r in range(8):
                below = [field[p, half + part * s + t, r] + slope_ratio * b for s, b in enumerate(below)]
                above = [field[p, part * s + part - 1 - t, 7 - r] + slope_ratio * a for s, a in enumerate(above)]
            return below, above

        zero = jnp.zeros((8, 128), f32)
        below, above = lax.fori_loop(0, part, step, ([zero] * split, [zero] * split))
        u, v = below[0], above[split - 1]
        jump = slope_ratio ** (8 * part)
        for s in range(1, split):
            u = below[s] + jump * u
            v = above[split - 1 - s] + jump * v
        top, bottom = field[p, tiles - 1, 7], field[p, 0, 0]
        for i, (a, b) in enumerate(((u, v), (top, bottom))):
            own[0, i, p] = a
            own[1, i, p] = b
            odd_out[i, p] = jnp.where(odd, a, b)
            even_out[i, p] = jnp.where(odd, b, a)
        flat = field.at[p].reshape(tiles * 64, 128)
        for t in range(tiles):
            sides[0, p, t] = flat[pl.ds(64 * t, 8, stride=8), :]
            sides[1, p, t] = flat[pl.ds(64 * t + 7, 8, stride=8), :]


def stencil():
    source = lax.broadcasted_iota(jnp.int32, (256, 256), 0) % 128
    target = lax.broadcasted_iota(jnp.int32, (256, 256), 1)
    offset = source - target % 128
    beyond = jnp.where(offset > 64, offset - 128, offset + 128)
    offset = jnp.where(target < 128, offset, beyond)
    size = jnp.abs(offset)
    value = jnp.where(size == 1, 45.0, jnp.where(size == 2, -9.0, jnp.where(size == 3, 1.0, 0.0)))
    return jnp.where(offset > 0, value, -value).astype(jnp.bfloat16)


def stream_kernel(field, sides, wall_hbm, out, wall, near, sems):
    planes, tiles = field.shape[0], field.shape[1]
    copies = sum([load_rows(wall_hbm, wall, sems, z) for z in range(wall.shape[0])], [])
    for copy in copies:
        copy.start()
    lane = lax.broadcasted_iota(jnp.int32, (8, 128), 1)
    piece = lax.broadcasted_iota(jnp.int32, (8, 128), 0)
    left = lane < 64
    outer = ((piece == 0) & left) | ((piece == 7) & (lane >= 64))
    matrix = stencil()

    def spread(x, columns):
        high = x.astype(jnp.bfloat16)
        low = (x - high.astype(f32)).astype(jnp.bfloat16)
        return jnp.dot(jnp.concatenate([high, low], axis=1), columns, preferred_element_type=f32)

    outside = spread(sides[...].reshape(2 * planes * tiles * 8, 128), matrix[:, 128:])
    after, before = outside[: planes * tiles * 8], outside[planes * tiles * 8 :]
    first = lax.broadcasted_iota(jnp.int32, before.shape, 1) < 64
    near[...] = jnp.where(first, before, after).reshape(planes, tiles, 8, 128)

    def body(g, carry):
        both = spread(field[pl.ds(g * TOGETHER, TOGETHER)].reshape(TOGETHER * tiles * 64, 128), matrix)
        for q in range(TOGETHER):
            p = g * TOGETHER + q
            for tile in range(tiles):
                for r in range(8):
                    at = (q * tiles + tile) * 64 + 8 * r
                    part = both[at : at + 8, 128:]
                    part = jnp.where(left, pltpu.roll(part, 1, 0), pltpu.roll(part, 7, 0))
                    part = jnp.where(outer, jnp.broadcast_to(near[p, tile, r : r + 1, :], (8, 128)), part)
                    speed = field[q % 2, tile, r] * (-1.0 / 60.0)
                    out[p, tile, r] = speed * (both[at : at + 8, :128] + part)
        return carry

    lax.fori_loop(0, planes // TOGETHER, body, 0)
    for copy in copies:
        copy.wait()


def sweep_kernel(
    coef, fading, field, stream, wall, own, odd_in, even_in, tend, work, total, odd1, even1, odd2, even2
):
    planes, tiles = field.shape[0], field.shape[1]
    count = planes // 2
    ks = range(count)
    here, first, last_block = place()
    odd = here % 2 == 1
    pair = (here // 2) % 2 == 1
    image = mix / kappa

    def below(i, p):
        inner = jnp.where(odd, even_in[i, p], odd_in[i, p])
        edge = slope_ratio * own[1, 0, p] - image * own[1, 1, p] if i == 0 else jnp.zeros((8, 128), f32)
        return jnp.where(first, edge, inner)

    def above(i, p):
        inner = jnp.where(odd, odd_in[i, p], even_in[i, p])
        edge = slope_ratio * own[0, 0, p] - image * own[0, 1, p] if i == 0 else jnp.zeros((8, 128), f32)
        return jnp.where(last_block, edge, inner)

    every = range(planes)
    ratio = [coef[k, 0] for k in ks]
    zero = jnp.zeros((8, 128), f32)

    def rise(t, u):
        for r in range(8):
            for p in every:
                work[p, t, r] = u[p]
            u = [field[p, t, r] + slope_ratio * u[p] for p in every]
        return u

    lax.fori_loop(0, tiles, rise, [below(0, p) for p in every])

    top, bottom = {}, {}
    for z in range(2):
        at = [2 * k + z for k in ks]
        ghost = [below(1, at[k]) for k in ks]

        def fall(i, carry, z=z, at=at, ghost=ghost):
            v, ahead, here, total, upper = carry
            t = tiles - 1 - i
            for r in range(7, -1, -1):
                speed = wall[z, t, r] * (-slope_gain)
                if r > 0:
                    last = [field[at[k], t, r - 1] for k in ks]
                else:
                    before = jnp.maximum(t - 1, 0)
                    last = [jnp.where(t == 0, ghost[k], field[at[k], before, 7]) for k in ks]
                slope = [
                    (work[at[k], t, r] - v[k]) + slope_edge * (last[k] - ahead[k]) for k in ks
                ]
                rate = [stream[at[k], t, r] + speed * slope[k] for k in ks]
                for k in ks:
                    tend[at[k], t, r] = rate[k]
                source = [rate[k] + 8.0 * here[k] for k in ks]
                grow = [jnp.broadcast_to(fading[k, i, 7 - r : 8 - r, :], (8, 128)) for k in ks]
                upper = [upper[k] + grow[k] * source[k] for k in ks]
                total = [source[k] + ratio[k] * total[k] for k in ks]
                for k in ks:
                    work[at[k], t, r] = total[k]
                v = [here[k] + slope_ratio * v[k] for k in ks]
                ahead, here = here, last
            return v, ahead, here, total, upper

        start = (
            [above(0, at[k]) for k in ks],
            [above(1, at[k]) for k in ks],
            [field[at[k], tiles - 1, 7] for k in ks],
            [zero] * count,
            [zero] * count,
        )
        lowest, upper = lax.fori_loop(0, tiles, fall, start)[3:]
        for k in ks:
            bottom[at[k]] = lowest[k]
            top[at[k]] = upper[k] / ratio[k]
    for p in every:
        weight, step = coef[p // 2, 3], ratio[p // 2]
        up, down = top[p], bottom[p]
        total[0, p] = up
        total[1, p] = down
        send_up = jnp.where(first, up - weight * step * down, up)
        send_down = jnp.where(last_block, down - weight * step * up, down)
        odd1[p] = jnp.where(odd, send_up, send_down)
        even1[p] = jnp.where(odd, send_down, send_up)
        odd2[p] = jnp.where(pair, send_up, send_down)
        even2[p] = jnp.where(pair, send_down, send_up)


def settle_kernel(coef, field, work, tend, tend_hbm, adv, sems):
    planes, tiles = field.shape[0], field.shape[1]
    every = range(planes)
    copies = sum([store_rows(tend, tend_hbm, sems, p) for p in every], [])
    for copy in copies:
        copy.start()
    ratio = [coef[k, 0] for k in range(planes // 2)]
    gain = [coef[k, 1] for k in range(planes // 2)]

    def settle(t, q):
        for r in range(8):
            q = [work[p, t, r] + ratio[p // 2] * q[p] for p in every]
            for p in every:
                adv[p, t, r] = gain[p // 2] * q[p] - field[p, t, r]
        return q

    lax.fori_loop(0, tiles, settle, [jnp.zeros((8, 128), f32)] * planes)
    for copy in copies:
        copy.wait()


def two_blocks(p, coef, total, odd1, even1, odd2, even2):
    here, first, last_block = place()
    odd = here % 2 == 1
    pair = (here // 2) % 2 == 1
    ratio, weight = coef[p // 2, 0], coef[p // 2, 3]
    low = jnp.where(odd, even1[p], odd1[p]) + weight * jnp.where(pair, even2[p], odd2[p])
    high = jnp.where(odd, odd1[p], even1[p]) + weight * jnp.where(pair, odd2[p], even2[p])
    end_low = -ratio * (total[1, p] + weight * high)
    end_high = -ratio * (total[0, p] + weight * low)
    return jnp.where(first, end_low, low), jnp.where(last_block, end_high, high)


def add_ends(k, lows, highs, fading, source, target):
    tiles = source.shape[1]

    def body(t, carry):
        for r in range(8):
            fade = jnp.broadcast_to(fading[k, t, r : r + 1, :], (8, 128))
            grow = jnp.broadcast_to(fading[k, tiles - 1 - t, 7 - r : 8 - r, :], (8, 128))
            for p, low, high in zip((2 * k, 2 * k + 1), lows, highs):
                target[p, t, r] = source[p, t, r] + (fade * low + grow * high)
        return carry

    lax.fori_loop(0, tiles, body, 0)


def finish_kernel(coef, fading, partial, total, odd1, even1, odd2, even2, out_hbm, out, sems):
    copies = []
    for k in range(coef.shape[0]):
        ratio, scale = coef[k, 0], coef[k, 5]
        lows, highs = [], []
        for p in (2 * k, 2 * k + 1):
            low, high = two_blocks(p, coef, total, odd1, even1, odd2, even2)
            lows.append(scale * (ratio * total[1, p] + low))
            highs.append(scale * high)
        add_ends(k, lows, highs, fading, partial, out)
        for p in (2 * k, 2 * k + 1):
            for copy in store_rows(out, out_hbm, sems, p):
                copy.start()
                copies.append(copy)
    for copy in copies:
        copy.wait()


def chain_kernel(coef, total, from_below, from_above, low_in, high_in, low_out, high_out, up_out, down_out):
    _, first, last_block = place()
    for p in range(total.shape[1]):
        ratio, weight = coef[p // 2, 0], coef[p // 2, 3]
        up, down = total[0, p], total[1, p]
        low = jnp.where(first, -ratio * (down + weight * high_in[p]), from_below[p])
        high = jnp.where(last_block, -ratio * (up + weight * low_in[p]), from_above[p])
        low_out[p] = low
        high_out[p] = high
        up_out[p] = up + weight * low
        down_out[p] = down + weight * high


def clear_kernel(*refs):
    for ref in refs:
        ref[...] = jnp.zeros(ref.shape, f32)


def chain_end_kernel(
    advanced_hbm, coef, fading, total, odd1, even1, odd2, even2, low, high, out_hbm, before, after, loads, stores
):
    for k in range(coef.shape[0]):
        pair = (2 * k, 2 * k + 1)
        scale = coef[k, 5]
        lows, highs = [], []
        for p in pair:
            near_low, near_high = two_blocks(p, coef, total, odd1, even1, odd2, even2)
            lows.append(scale * (low[p] - near_low))
            highs.append(scale * (high[p] - near_high))
        copies = sum([load_rows(advanced_hbm, before, loads, p) for p in pair], [])
        for copy in copies:
            copy.start()
        for copy in copies:
            copy.wait()
        add_ends(k, lows, highs, fading, before, after)
        copies = sum([store_rows(after, out_hbm, stores, p) for p in pair], [])
        for copy in copies:
            copy.start()
        for copy in copies:
            copy.wait()


VMEM = pl.BlockSpec(memory_space=pltpu.VMEM)
SMEM = pl.BlockSpec(memory_space=pltpu.SMEM)
ANY = pl.BlockSpec(memory_space=pl.ANY)


def pairs(count, by, odd):
    found = []
    for a in range(count - by):
        if (a // by) % 2 == odd:
            found += [(a, a + by), (a + by, a)]
    return found


def row_shape(shape):
    planes, tiles = shape[:2]
    return (planes, tiles, 8, 8, 128)


def exchange(odd, even, by):
    count = lax.axis_size("wall")
    return (
        lax.ppermute(odd, "wall", pairs(count, by, 1)),
        lax.ppermute(even, "wall", pairs(count, by, 0)),
    )


def whole_chain(advanced, coef, fading, total, *arrived):
    count = lax.axis_size("wall")
    rise = [(i, i + 1) for i in range(count - 1)]
    fall = [(i + 1, i) for i in range(count - 1)]
    rows = jax.ShapeDtypeStruct(total.shape[1:], f32)
    planes = advanced.shape[0]

    def step(_, carry):
        low, high, up, down = carry
        return list(pl.pallas_call(
            chain_kernel,
            in_specs=[VMEM] * 6,
            out_specs=[VMEM] * 4,
            out_shape=[rows] * 4,
            compiler_params=params(2),
            name="chain",
        )(coef, total, lax.ppermute(up, "wall", rise), lax.ppermute(down, "wall", fall), low, high))

    start = list(pl.pallas_call(
        clear_kernel,
        out_specs=[VMEM] * 4,
        out_shape=[rows] * 4,
        compiler_params=params(2),
        name="chain_start",
    )())
    low, high, _, _ = lax.fori_loop(0, 2 * count, step, start)
    return pl.pallas_call(
        chain_end_kernel,
        in_specs=[ANY] + [VMEM] * 9,
        out_specs=ANY,
        out_shape=jax.ShapeDtypeStruct(advanced.shape, f32),
        scratch_shapes=[pltpu.VMEM(row_shape(advanced.shape), f32)] * 2 + [pltpu.SemaphoreType.DMA((planes, 8))] * 2,
        compiler_params=params(18),
        name="chain_end",
    )(advanced, coef, fading, total, *arrived, low, high)


def on_device(fields, wall_velocity, diffusion):
    count, depth, height, width = fields.shape
    planes, tiles = count * depth, height // 8
    shape = jax.ShapeDtypeStruct
    source, wall_source = lines(fields), lines(wall_velocity)
    full = row_shape(source.shape)
    resident = pltpu.VMEM(full, f32)
    rows = shape((planes, 8, 128), f32)
    ends = shape((2, planes, 8, 128), f32)
    in_hbm = functools.partial(pltpu.with_memory_space_constraint, memory_space=pltpu.HBM)
    plane_sems = pltpu.SemaphoreType.DMA((planes, 8))

    field, sides, own, odd, even, coef, fading, flag = pl.pallas_call(
        edges_kernel,
        in_specs=[ANY, ANY],
        out_specs=[VMEM] * 7 + [SMEM],
        out_shape=[
            resident,
            shape((2, planes, tiles, 8, 128), f32),
            pltpu.VMEM((2, 2, planes, 8, 128), f32),
            ends,
            ends,
            pltpu.VMEM((count, 6, 8, 128), f32),
            pltpu.VMEM((count, tiles, 8, 128), f32),
            shape((1,), jnp.int32),
        ],
        scratch_shapes=[pltpu.SMEM((count,), f32), plane_sems, pltpu.SemaphoreType.DMA],
        compiler_params=params(4),
        name="edges",
    )(in_hbm(source), in_hbm(diffusion))
    sides = lax.ppermute(sides, "stream", [(0, 1), (1, 0)])
    odd, even = exchange(odd, even, 1)

    stream, wall = pl.pallas_call(
        stream_kernel,
        in_specs=[VMEM, VMEM, ANY],
        out_specs=[VMEM] * 2,
        out_shape=[resident, pltpu.VMEM(row_shape(wall_source.shape), f32)],
        scratch_shapes=[pltpu.VMEM((planes, tiles, 8, 128), f32), pltpu.SemaphoreType.DMA((depth, 8))],
        compiler_params=params(12),
        cost_estimate=pl.CostEstimate(flops=4_000_000_000, transcendentals=0, bytes_accessed=0),
        name="streamwise",
    )(field, sides, in_hbm(wall_source))

    rate, work, total, *sent = pl.pallas_call(
        sweep_kernel,
        in_specs=[VMEM] * 8,
        out_specs=[VMEM] * 7,
        out_shape=[resident, resident, pltpu.VMEM((2, planes, 8, 128), f32)] + [rows] * 4,
        compiler_params=params(2),
        name="sweeps",
    )(coef, fading, field, stream, wall, own, odd, even)

    odd1, even1, odd2, even2 = sent
    far = exchange(odd2, even2, 2)
    near = exchange(odd1, even1, 1)
    arrived = [*near, *far]

    tendency, partial = pl.pallas_call(
        settle_kernel,
        in_specs=[VMEM] * 4,
        out_specs=[ANY, VMEM],
        out_shape=[shape(source.shape, f32), resident],
        scratch_shapes=[plane_sems],
        compiler_params=params(2),
        cost_estimate=pl.CostEstimate(flops=4_000_000_000, transcendentals=0, bytes_accessed=0),
        name="settle",
    )(coef, field, work, rate)

    advanced = pl.pallas_call(
        finish_kernel,
        in_specs=[VMEM] * 8,
        out_specs=ANY,
        out_shape=shape(source.shape, f32),
        scratch_shapes=[pltpu.VMEM(full, f32), plane_sems],
        compiler_params=params(10),
        name="finish",
    )(coef, fading, partial, total, *arrived)
    advanced = lax.cond(flag[0] != 0, whole_chain, lambda x, *_: x, advanced, coef, fading, total, *arrived)
    return unlines(tendency, fields.shape), unlines(advanced, fields.shape)


def solution(mesh):
    tall = P(None, None, "wall", "stream")
    return jax.shard_map(
        on_device,
        mesh=mesh,
        in_specs=(tall, P(None, "wall", "stream"), P()),
        out_specs=(tall, tall),
        check_vma=False,
    )
```

```python
import functools
import math

import jax
import jax.numpy as jnp
from jax import lax
from jax.experimental import pallas as pl
from jax.experimental.pallas import tpu as pltpu
from jax.sharding import PartitionSpec as P

time_step = 0.25
compact_alpha = 1.0 / 3.0
compact_near = 14.0 / 9.0
compact_far = 1.0 / 9.0
slope_ratio = (math.sqrt(1.0 - 4.0 * compact_alpha**2) - 1.0) / (2.0 * compact_alpha)
mix = 0.25 * compact_far / compact_alpha
rest = 0.5 * compact_near - mix
green = 1.0 / (1.0 + 2.0 * compact_alpha * slope_ratio)
kappa = rest * green * (slope_ratio - 1.0 / slope_ratio)
slope_gain = kappa * slope_ratio
slope_edge = -mix / slope_gain
tiny = 1.1754943508222875e-38
SPLIT = 6
TOGETHER = 2
f32 = jnp.float32
MIB = 1 << 20


def params(mib):
    return pltpu.CompilerParams(vmem_limit_bytes=mib * MIB)


def lines(x):
    rows, cols = x.shape[-2:]
    y = x.reshape(-1, rows // 8, 8, cols // 128, 128)
    return jnp.swapaxes(y, 2, 3)[:, :, :, :, None, :]


def unlines(y, shape):
    return jnp.swapaxes(y[:, :, :, :, 0, :], 2, 3).reshape(shape)


def load_rows(hbm, rows, sems, p):
    return [
        pltpu.make_async_copy(hbm.at[p, :, :, r, 0], rows.at[p, :, r], sems.at[p, r]) for r in range(8)
    ]


def store_rows(rows, hbm, sems, p):
    return [
        pltpu.make_async_copy(rows.at[p, :, r], hbm.at[p, :, :, r, 0], sems.at[p, r]) for r in range(8)
    ]


def place():
    here = lax.axis_index("wall")
    return here, here == 0, here == lax.axis_size("wall") - 1


def carries_near():
    return lax.axis_index("stream") == 0


def edges_kernel(field_hbm, diffusion_hbm, field, sides, own, odd_out, even_out, coef, fading, flag, rate, sems, sem):
    planes, tiles = field.shape[0], field.shape[1]
    half = tiles // 2
    split = SPLIT
    part = half // split
    rates = pltpu.make_async_copy(diffusion_hbm, rate, sem)
    rates.start()
    copies = [load_rows(field_hbm, field, sems, p) for p in range(planes)]
    for copy in sum(copies, []):
        copy.start()
    odd = place()[0] % 2 == 1

    def coefficients():
        rates.wait()
        longest = jnp.zeros((8, 128), f32)
        for k in range(rate.shape[0]):
            d = jnp.full((8, 128), rate[k])
            larger = 0.5 * (1.0 + 2.0 * d + jnp.sqrt(1.0 + 4.0 * d))
            ratio = d / larger
            log_ratio = jnp.log(ratio)
            weight = jnp.exp(8.0 * tiles * log_ratio)
            damp = 1.0 - ratio * ratio
            gain = time_step / larger
            for i, value in enumerate((ratio, gain, damp, weight, log_ratio, gain / damp)):
                coef[k, i] = value
            longest = jnp.maximum(longest, weight)
            line = lax.broadcasted_iota(jnp.int32, (8, 128), 0).astype(f32) + 1.0
            for tile in range(tiles):
                fading[k, tile] = jnp.exp(log_ratio * (line + 8.0 * tile))
        flag[0] = (jnp.max(longest * longest) >= tiny).astype(jnp.int32)

    for p in range(planes):
        for copy in copies[p]:
            copy.wait()
        if p == planes // 2:
            coefficients()

        def step(t, carry, p=p):
            below, above = carry
            for r in range(8):
                below = [field[p, half + part * s + t, r] + slope_ratio * b for s, b in enumerate(below)]
                above = [field[p, part * s + part - 1 - t, 7 - r] + slope_ratio * a for s, a in enumerate(above)]
            return below, above

        zero = jnp.zeros((8, 128), f32)
        below, above = lax.fori_loop(0, part, step, ([zero] * split, [zero] * split))
        u, v = below[0], above[split - 1]
        jump = slope_ratio ** (8 * part)
        for s in range(1, split):
            u = below[s] + jump * u
            v = above[split - 1 - s] + jump * v
        top, bottom = field[p, tiles - 1, 7], field[p, 0, 0]
        for i, (a, b) in enumerate(((u, v), (top, bottom))):
            own[0, i, p] = a
            own[1, i, p] = b
            odd_out[i, p] = jnp.where(odd, a, b)
            even_out[i, p] = jnp.where(odd, b, a)
        flat = field.at[p].reshape(tiles * 64, 128)
        for t in range(tiles):
            sides[0, p, t] = flat[pl.ds(64 * t, 8, stride=8), :]
            sides[1, p, t] = flat[pl.ds(64 * t + 7, 8, stride=8), :]


def stencil():
    source = lax.broadcasted_iota(jnp.int32, (256, 256), 0) % 128
    target = lax.broadcasted_iota(jnp.int32, (256, 256), 1)
    offset = source - target % 128
    beyond = jnp.where(offset > 64, offset - 128, offset + 128)
    offset = jnp.where(target < 128, offset, beyond)
    size = jnp.abs(offset)
    value = jnp.where(size == 1, 45.0, jnp.where(size == 2, -9.0, jnp.where(size == 3, 1.0, 0.0)))
    return jnp.where(offset > 0, value, -value).astype(jnp.bfloat16)


def stream_kernel(field, sides, wall_hbm, out, wall, near, sems):
    planes, tiles = field.shape[0], field.shape[1]
    copies = sum([load_rows(wall_hbm, wall, sems, z) for z in range(wall.shape[0])], [])
    for copy in copies:
        copy.start()
    lane = lax.broadcasted_iota(jnp.int32, (8, 128), 1)
    piece = lax.broadcasted_iota(jnp.int32, (8, 128), 0)
    left = lane < 64
    outer = ((piece == 0) & left) | ((piece == 7) & (lane >= 64))
    matrix = stencil()

    def spread(x, columns):
        high = x.astype(jnp.bfloat16)
        low = (x - high.astype(f32)).astype(jnp.bfloat16)
        return jnp.dot(jnp.concatenate([high, low], axis=1), columns, preferred_element_type=f32)

    outside = spread(sides[...].reshape(2 * planes * tiles * 8, 128), matrix[:, 128:])
    after, before = outside[: planes * tiles * 8], outside[planes * tiles * 8 :]
    first = lax.broadcasted_iota(jnp.int32, before.shape, 1) < 64
    near[...] = jnp.where(first, before, after).reshape(planes, tiles, 8, 128)

    def body(g, carry):
        both = spread(field[pl.ds(g * TOGETHER, TOGETHER)].reshape(TOGETHER * tiles * 64, 128), matrix)
        for q in range(TOGETHER):
            p = g * TOGETHER + q
            for tile in range(tiles):
                for r in range(8):
                    at = (q * tiles + tile) * 64 + 8 * r
                    part = both[at : at + 8, 128:]
                    part = jnp.where(left, pltpu.roll(part, 1, 0), pltpu.roll(part, 7, 0))
                    part = jnp.where(outer, jnp.broadcast_to(near[p, tile, r : r + 1, :], (8, 128)), part)
                    speed = field[q % 2, tile, r] * (-1.0 / 60.0)
                    out[p, tile, r] = speed * (both[at : at + 8, :128] + part)
        return carry

    lax.fori_loop(0, planes // TOGETHER, body, 0)
    for copy in copies:
        copy.wait()


def sweep_kernel(
    coef, fading, field, stream, wall, own, odd_in, even_in, tend, work, total, keep, give
):
    planes, tiles = field.shape[0], field.shape[1]
    count = planes // 2
    ks = range(count)
    here, first, last_block = place()
    odd = here % 2 == 1
    pair = (here // 2) % 2 == 1
    image = mix / kappa

    def below(i, p):
        inner = jnp.where(odd, even_in[i, p], odd_in[i, p])
        edge = slope_ratio * own[1, 0, p] - image * own[1, 1, p] if i == 0 else jnp.zeros((8, 128), f32)
        return jnp.where(first, edge, inner)

    def above(i, p):
        inner = jnp.where(odd, odd_in[i, p], even_in[i, p])
        edge = slope_ratio * own[0, 0, p] - image * own[0, 1, p] if i == 0 else jnp.zeros((8, 128), f32)
        return jnp.where(last_block, edge, inner)

    every = range(planes)
    ratio = [coef[k, 0] for k in ks]
    zero = jnp.zeros((8, 128), f32)

    def rise(t, u):
        for r in range(8):
            for p in every:
                work[p, t, r] = u[p]
            u = [field[p, t, r] + slope_ratio * u[p] for p in every]
        return u

    lax.fori_loop(0, tiles, rise, [below(0, p) for p in every])

    top, bottom = {}, {}
    for z in range(2):
        at = [2 * k + z for k in ks]
        ghost = [below(1, at[k]) for k in ks]

        def fall(i, carry, z=z, at=at, ghost=ghost):
            v, ahead, here, total, upper = carry
            t = tiles - 1 - i
            for r in range(7, -1, -1):
                speed = wall[z, t, r] * (-slope_gain)
                if r > 0:
                    last = [field[at[k], t, r - 1] for k in ks]
                else:
                    before = jnp.maximum(t - 1, 0)
                    last = [jnp.where(t == 0, ghost[k], field[at[k], before, 7]) for k in ks]
                slope = [
                    (work[at[k], t, r] - v[k]) + slope_edge * (last[k] - ahead[k]) for k in ks
                ]
                rate = [stream[at[k], t, r] + speed * slope[k] for k in ks]
                for k in ks:
                    tend[at[k], t, r] = rate[k]
                source = [rate[k] + 8.0 * here[k] for k in ks]
                grow = [jnp.broadcast_to(fading[k, i, 7 - r : 8 - r, :], (8, 128)) for k in ks]
                upper = [upper[k] + grow[k] * source[k] for k in ks]
                total = [source[k] + ratio[k] * total[k] for k in ks]
                for k in ks:
                    work[at[k], t, r] = total[k]
                v = [here[k] + slope_ratio * v[k] for k in ks]
                ahead, here = here, last
            return v, ahead, here, total, upper

        start = (
            [above(0, at[k]) for k in ks],
            [above(1, at[k]) for k in ks],
            [field[at[k], tiles - 1, 7] for k in ks],
            [zero] * count,
            [zero] * count,
        )
        lowest, upper = lax.fori_loop(0, tiles, fall, start)[3:]
        for k in ks:
            bottom[at[k]] = lowest[k]
            top[at[k]] = upper[k] / ratio[k]
    for p in every:
        weight, step = coef[p // 2, 3], ratio[p // 2]
        up, down = top[p], bottom[p]
        total[0, p] = up
        total[1, p] = down
        send_up = jnp.where(first, up - weight * step * down, up)
        send_down = jnp.where(last_block, down - weight * step * up, down)
        near = jnp.where(odd, send_up, send_down), jnp.where(odd, send_down, send_up)
        far = jnp.where(pair, send_up, send_down), jnp.where(pair, send_down, send_up)
        for i in range(2):
            keep[i, p] = jnp.where(carries_near(), near[i], far[i])
            give[i, p] = jnp.where(carries_near(), far[i], near[i])


def pack_kernel(keep, got, odd, even):
    for i, target in enumerate((odd, even)):
        target[0] = keep[i]
        target[1] = got[i]


def settle_kernel(coef, field, work, tend, tend_hbm, adv, sems):
    planes, tiles = field.shape[0], field.shape[1]
    every = range(planes)
    copies = sum([store_rows(tend, tend_hbm, sems, p) for p in every], [])
    for copy in copies:
        copy.start()
    ratio = [coef[k, 0] for k in range(planes // 2)]
    gain = [coef[k, 1] for k in range(planes // 2)]

    def settle(t, q):
        for r in range(8):
            q = [work[p, t, r] + ratio[p // 2] * q[p] for p in every]
            for p in every:
                adv[p, t, r] = gain[p // 2] * q[p] - field[p, t, r]
        return q

    lax.fori_loop(0, tiles, settle, [jnp.zeros((8, 128), f32)] * planes)
    for copy in copies:
        copy.wait()


def two_blocks(p, coef, total, odd_own, even_own, odd_other, even_other):
    here, first, last_block = place()
    odd = here % 2 == 1
    pair = (here // 2) % 2 == 1
    mine, other = (odd_own[0, p], even_own[0, p]), (odd_other[1, p], even_other[1, p])
    odd1, even1 = [jnp.where(carries_near(), a, b) for a, b in zip(mine, other)]
    odd2, even2 = [jnp.where(carries_near(), b, a) for a, b in zip(mine, other)]
    ratio, weight = coef[p // 2, 0], coef[p // 2, 3]
    low = jnp.where(odd, even1, odd1) + weight * jnp.where(pair, even2, odd2)
    high = jnp.where(odd, odd1, even1) + weight * jnp.where(pair, odd2, even2)
    end_low = -ratio * (total[1, p] + weight * high)
    end_high = -ratio * (total[0, p] + weight * low)
    return jnp.where(first, end_low, low), jnp.where(last_block, end_high, high)


def add_ends(k, lows, highs, fading, source, target):
    tiles = source.shape[1]

    def body(t, carry):
        for r in range(8):
            fade = jnp.broadcast_to(fading[k, t, r : r + 1, :], (8, 128))
            grow = jnp.broadcast_to(fading[k, tiles - 1 - t, 7 - r : 8 - r, :], (8, 128))
            for p, low, high in zip((2 * k, 2 * k + 1), lows, highs):
                target[p, t, r] = source[p, t, r] + (fade * low + grow * high)
        return carry

    lax.fori_loop(0, tiles, body, 0)


def finish_kernel(coef, fading, partial, total, odd_own, even_own, odd_other, even_other, out_hbm, out, sems):
    copies = []
    for k in range(coef.shape[0]):
        ratio, scale = coef[k, 0], coef[k, 5]
        lows, highs = [], []
        for p in (2 * k, 2 * k + 1):
            low, high = two_blocks(p, coef, total, odd_own, even_own, odd_other, even_other)
            lows.append(scale * (ratio * total[1, p] + low))
            highs.append(scale * high)
        add_ends(k, lows, highs, fading, partial, out)
        for p in (2 * k, 2 * k + 1):
            for copy in store_rows(out, out_hbm, sems, p):
                copy.start()
                copies.append(copy)
    for copy in copies:
        copy.wait()


def chain_kernel(coef, total, from_below, from_above, low_in, high_in, low_out, high_out, up_out, down_out):
    _, first, last_block = place()
    for p in range(total.shape[1]):
        ratio, weight = coef[p // 2, 0], coef[p // 2, 3]
        up, down = total[0, p], total[1, p]
        low = jnp.where(first, -ratio * (down + weight * high_in[p]), from_below[p])
        high = jnp.where(last_block, -ratio * (up + weight * low_in[p]), from_above[p])
        low_out[p] = low
        high_out[p] = high
        up_out[p] = up + weight * low
        down_out[p] = down + weight * high


def clear_kernel(*refs):
    for ref in refs:
        ref[...] = jnp.zeros(ref.shape, f32)


def chain_end_kernel(
    advanced_hbm,
    coef,
    fading,
    total,
    odd_own,
    even_own,
    odd_other,
    even_other,
    low,
    high,
    out_hbm,
    before,
    after,
    loads,
    stores,
):
    for k in range(coef.shape[0]):
        pair = (2 * k, 2 * k + 1)
        scale = coef[k, 5]
        lows, highs = [], []
        for p in pair:
            near_low, near_high = two_blocks(p, coef, total, odd_own, even_own, odd_other, even_other)
            lows.append(scale * (low[p] - near_low))
            highs.append(scale * (high[p] - near_high))
        copies = sum([load_rows(advanced_hbm, before, loads, p) for p in pair], [])
        for copy in copies:
            copy.start()
        for copy in copies:
            copy.wait()
        add_ends(k, lows, highs, fading, before, after)
        copies = sum([store_rows(after, out_hbm, stores, p) for p in pair], [])
        for copy in copies:
            copy.start()
        for copy in copies:
            copy.wait()


VMEM = pl.BlockSpec(memory_space=pltpu.VMEM)
SMEM = pl.BlockSpec(memory_space=pltpu.SMEM)
ANY = pl.BlockSpec(memory_space=pl.ANY)


def pairs(count, by, odd):
    found = []
    for a in range(count - by):
        if (a // by) % 2 == odd:
            found += [(a, a + by), (a + by, a)]
    return found


def row_shape(shape):
    planes, tiles = shape[:2]
    return (planes, tiles, 8, 8, 128)


def swap(x):
    return lax.ppermute(x, "stream", [(0, 1), (1, 0)])


def carried(x, odd):
    count, cores = lax.axis_size("wall"), lax.axis_size("stream")
    moves = [(cores * a + c, cores * b + c) for c in range(cores) for a, b in pairs(count, c + 1, odd)]
    return lax.ppermute(x, ("wall", "stream"), moves)


def whole_chain(advanced, coef, fading, total, *arrived):
    count = lax.axis_size("wall")
    rise = [(i, i + 1) for i in range(count - 1)]
    fall = [(i + 1, i) for i in range(count - 1)]
    rows = jax.ShapeDtypeStruct(total.shape[1:], f32)
    planes = advanced.shape[0]

    def step(_, carry):
        low, high, up, down = carry
        return list(pl.pallas_call(
            chain_kernel,
            in_specs=[VMEM] * 6,
            out_specs=[VMEM] * 4,
            out_shape=[rows] * 4,
            compiler_params=params(2),
            name="chain",
        )(coef, total, lax.ppermute(up, "wall", rise), lax.ppermute(down, "wall", fall), low, high))

    start = list(pl.pallas_call(
        clear_kernel,
        out_specs=[VMEM] * 4,
        out_shape=[rows] * 4,
        compiler_params=params(2),
        name="chain_start",
    )())
    low, high, _, _ = lax.fori_loop(0, 2 * count, step, start)
    return pl.pallas_call(
        chain_end_kernel,
        in_specs=[ANY] + [VMEM] * 9,
        out_specs=ANY,
        out_shape=jax.ShapeDtypeStruct(advanced.shape, f32),
        scratch_shapes=[pltpu.VMEM(row_shape(advanced.shape), f32)] * 2 + [pltpu.SemaphoreType.DMA((planes, 8))] * 2,
        compiler_params=params(18),
        name="chain_end",
    )(advanced, coef, fading, total, *arrived, low, high)


def on_device(fields, wall_velocity, diffusion):
    count, depth, height, width = fields.shape
    planes, tiles = count * depth, height // 8
    shape = jax.ShapeDtypeStruct
    source, wall_source = lines(fields), lines(wall_velocity)
    full = row_shape(source.shape)
    resident = pltpu.VMEM(full, f32)
    ends = shape((2, planes, 8, 128), f32)
    in_hbm = functools.partial(pltpu.with_memory_space_constraint, memory_space=pltpu.HBM)
    plane_sems = pltpu.SemaphoreType.DMA((planes, 8))

    field, sides, own, odd, even, coef, fading, flag = pl.pallas_call(
        edges_kernel,
        in_specs=[ANY, ANY],
        out_specs=[VMEM] * 7 + [SMEM],
        out_shape=[
            resident,
            shape((2, planes, tiles, 8, 128), f32),
            pltpu.VMEM((2, 2, planes, 8, 128), f32),
            ends,
            ends,
            pltpu.VMEM((count, 6, 8, 128), f32),
            pltpu.VMEM((count, tiles, 8, 128), f32),
            shape((1,), jnp.int32),
        ],
        scratch_shapes=[pltpu.SMEM((count,), f32), plane_sems, pltpu.SemaphoreType.DMA],
        compiler_params=params(4),
        name="edges",
    )(in_hbm(source), in_hbm(diffusion))
    sides = swap(sides)
    blocks = lax.axis_size("wall")
    odd = lax.ppermute(odd, "wall", pairs(blocks, 1, 1))
    even = lax.ppermute(even, "wall", pairs(blocks, 1, 0))

    stream, wall = pl.pallas_call(
        stream_kernel,
        in_specs=[VMEM, VMEM, ANY],
        out_specs=[VMEM] * 2,
        out_shape=[resident, pltpu.VMEM(row_shape(wall_source.shape), f32)],
        scratch_shapes=[pltpu.VMEM((planes, tiles, 8, 128), f32), pltpu.SemaphoreType.DMA((depth, 8))],
        compiler_params=params(12),
        cost_estimate=pl.CostEstimate(flops=4_000_000_000, transcendentals=0, bytes_accessed=0),
        name="streamwise",
    )(field, sides, in_hbm(wall_source))

    rate, work, total, keep, give = pl.pallas_call(
        sweep_kernel,
        in_specs=[VMEM] * 8,
        out_specs=[VMEM] * 5,
        out_shape=[resident, resident, pltpu.VMEM((2, planes, 8, 128), f32), pltpu.VMEM((2, planes, 8, 128), f32), ends],
        compiler_params=params(2),
        name="sweeps",
    )(coef, fading, field, stream, wall, own, odd, even)

    odd, even = pl.pallas_call(
        pack_kernel,
        in_specs=[VMEM] * 2,
        out_specs=[VMEM] * 2,
        out_shape=[ends] * 2,
        compiler_params=params(2),
        name="pack",
    )(keep, swap(give))
    odd, even = carried(odd, 1), carried(even, 0)

    tendency, partial = pl.pallas_call(
        settle_kernel,
        in_specs=[VMEM] * 4,
        out_specs=[ANY, VMEM],
        out_shape=[shape(source.shape, f32), resident],
        scratch_shapes=[plane_sems],
        compiler_params=params(2),
        cost_estimate=pl.CostEstimate(flops=4_000_000_000, transcendentals=0, bytes_accessed=0),
        name="settle",
    )(coef, field, work, rate)
    odd, even, partial = lax.optimization_barrier((odd, even, partial))
    arrived = [odd, even, swap(odd), swap(even)]

    advanced = pl.pallas_call(
        finish_kernel,
        in_specs=[VMEM] * 8,
        out_specs=ANY,
        out_shape=shape(source.shape, f32),
        scratch_shapes=[pltpu.VMEM(full, f32), plane_sems],
        compiler_params=params(10),
        name="finish",
    )(coef, fading, partial, total, *arrived)
    advanced = lax.cond(flag[0] != 0, whole_chain, lambda x, *_: x, advanced, coef, fading, total, *arrived)
    return unlines(tendency, fields.shape), unlines(advanced, fields.shape)


def solution(mesh):
    tall = P(None, None, "wall", "stream")
    return jax.shard_map(
        on_device,
        mesh=mesh,
        in_specs=(tall, P(None, "wall", "stream"), P()),
        out_specs=(tall, tall),
        check_vma=False,
    )
```
